32 devices in a mesh: mix: 4 (over z), span: 8 (over y, x, core).
Axes of the slice: x: 2, y: 2, z: 4, core: 2. Of those that a mesh axis runs over, the one named last changes fastest.
Arguments:
- mixture: bfloat16 [512, 256, 256], P(('mix', 'span')), parts along dimension 0, may hold values from -16 to 16, as said below
- w_query: bfloat16 [2, 256, 256], replicated, may hold values from -4 to 4
- w_key: bfloat16 [2, 256, 256], replicated, may hold values from -4 to 4
- w_value: bfloat16 [2, 256, 256], replicated, may hold values from -0.375 to 0.375
- w_out: bfloat16 [2, 256, 256], replicated, may hold values from -0.375 to 0.375
- w_up: bfloat16 [2, 256, 1024], replicated, may hold values from -0.375 to 0.375
- w_down: bfloat16 [2, 1024, 256], replicated, may hold values from -0.1875 to 0.1875
- ln_gain: float32 [2, 2, 256], replicated, may hold values from 0.25 to 1.75
- gln_gain: float32 [2, 256], replicated, may hold values from 0.25 to 1.75
- gln_bias: float32 [2, 256], replicated, may hold values from -3 to 3
Outputs:
- block_out: bfloat16 [512, 256, 256], P(('mix', 'span')), parts along dimension 0
The draws below stay inside these ranges and needn't reach their ends.
There are 4 independent parts, one for each index of `mix`. The reference program is written for one: setup_inputs(seed, part) draws one part's arguments, and reference() takes and returns one part's arrays. A program takes and returns all parts, laid end to end along the dimension named above; an argument that names none is the same for every part. Nothing has to cross between parts.
Inputs may be any that keep to these rules, and one draw needn't show every extreme that they name: `mixture`: entries of order one, scaled by a factor per segment.
All inputs are finite; a program needn't handle non-finite values.
Results may differ from the reference program's by a relative error of at most 0.0057.
Values may be sent and summed in bfloat16 or wider, within the bound.
A program may use at most 128 MiB of HBM per device.

```python
import math
import jax
import jax.numpy as jnp
from jax import lax

D = 256
HEADS = 8
FF = 1024
FRAMES = 256
SEGMENTS = 128


def draw_mixture(key, part):
    keys = jax.random.split(key, 4)
    scales = jnp.exp(jax.random.uniform(keys[0], (SEGMENTS, 1, 1), jnp.float32, math.log(0.25), math.log(4.0)))
    offsets = 0.5 * jax.random.normal(keys[1], (SEGMENTS, 1, 1), jnp.float32)
    result = offsets + scales * jax.random.normal(keys[2], (SEGMENTS, FRAMES, D), jnp.float32)
    return jnp.clip(result, -16.0, 16.0).astype(jnp.bfloat16)


def query_key_pair(key):
    base = jax.random.normal(jax.random.fold_in(key, 11), (2, D, D), jnp.float32) * D ** (-0.5)
    other = jax.random.normal(jax.random.fold_in(key, 12), (2, D, D), jnp.float32) * D ** (-0.5)
    return (jnp.clip(base, -4.0, 4.0), jnp.clip(other, -4.0, 4.0))


def draw_w_query(key, part):
    return query_key_pair(key)[0].astype(jnp.bfloat16)


def draw_w_key(key, part):
    return query_key_pair(key)[1].astype(jnp.bfloat16)


def normal_values(rng, dims, scale, reach, kind=jnp.bfloat16):
    entries = scale * jax.random.normal(rng, dims, jnp.float32)
    return jnp.clip(entries, min=-reach, max=reach).astype(kind)


def setup_inputs(seed: int = 0, part: int = 0) -> dict:
    arg_keys = jax.random.split(jax.random.key(seed), 11)
    own_keys = jax.random.split(jax.random.fold_in(arg_keys[10], part), 11)
    mixture = draw_mixture(jax.random.fold_in(jax.random.fold_in(arg_keys[10], part), 71), part)
    w_query = draw_w_query(jax.random.fold_in(arg_keys[10], 71), part)
    w_key = draw_w_key(jax.random.fold_in(arg_keys[10], 71), part)
    w_value = normal_values(arg_keys[3], (2, D, D), D ** -0.5, 0.375)
    w_out = normal_values(arg_keys[4], (2, D, D), D ** -0.5, 0.375)
    w_up = normal_values(arg_keys[5], (2, D, FF), D ** -0.5, 0.375)
    w_down = normal_values(arg_keys[6], (2, FF, D), FF ** -0.5, 0.1875)
    ln_gain = jnp.clip(1.0 + 0.15 * jax.random.normal(arg_keys[7], (2, 2, D), jnp.float32), 0.25, 1.75)
    gln_gain = jnp.clip(1.0 + 0.15 * jax.random.normal(arg_keys[8], (2, D), jnp.float32), 0.25, 1.75)
    gln_bias = normal_values(arg_keys[9], (2, D), 0.5, 3.0, jnp.float32)
    return {"mixture": mixture, "w_query": w_query, "w_key": w_key, "w_value": w_value, "w_out": w_out, "w_up": w_up, "w_down": w_down, "ln_gain": ln_gain, "gln_gain": gln_gain, "gln_bias": gln_bias}


norm_eps = 1e-05

def pos_table(length, width):
    places = jnp.arange(length, dtype=jnp.float32)[:, None]
    column = jnp.arange(width)
    rates = jnp.exp(-(2 * (column // 2)).astype(jnp.float32) / width * math.log(10000.0))
    angles = places * rates[None, :]
    return jnp.where((column % 2 == 0)[None, :], jnp.sin(angles), jnp.cos(angles))

def norm_rows(rows, gain):
    center = lax.optimization_barrier(jnp.mean(rows, axis=-1, keepdims=True))
    shifted = rows - center
    spread = lax.optimization_barrier(jnp.mean(shifted * shifted, axis=-1, keepdims=True))
    return shifted * lax.rsqrt(spread + norm_eps) * gain

def attend(queries, key_rows, values):
    length = queries.shape[0]
    split_q = queries.reshape(length, HEADS, D // HEADS).astype(jnp.float32)
    split_k = key_rows.reshape(length, HEADS, D // HEADS).astype(jnp.float32)
    split_v = values.reshape(length, HEADS, D // HEADS).astype(jnp.float32)
    scores = jnp.einsum('qhd,khd->hqk', split_q, split_k) / math.sqrt(D // HEADS)
    weights = jax.nn.softmax(scores, axis=-1).astype(jnp.bfloat16)
    context = jnp.einsum('hqk,khd->qhd', weights.astype(jnp.float32), split_v)
    return context.astype(jnp.bfloat16).reshape(length, D)

def encoder_layer(sequence, level, w_query, w_key, w_value, w_out, w_up, w_down, ln_gain):
    length = sequence.shape[0]
    inputs = sequence.astype(jnp.float32) + pos_table(length, D)
    normed = norm_rows(inputs, ln_gain[level, 0]).astype(jnp.bfloat16)
    queries = jnp.dot(normed, w_query[level], preferred_element_type=jnp.float32).astype(jnp.bfloat16)
    key_rows = jnp.dot(normed, w_key[level], preferred_element_type=jnp.float32).astype(jnp.bfloat16)
    values = jnp.dot(normed, w_value[level], preferred_element_type=jnp.float32).astype(jnp.bfloat16)
    context = attend(queries, key_rows, values)
    after_attn = inputs + jnp.dot(context, w_out[level], preferred_element_type=jnp.float32)
    normed_two = norm_rows(after_attn, ln_gain[level, 1]).astype(jnp.bfloat16)
    hidden = jax.nn.relu(jnp.dot(normed_two, w_up[level], preferred_element_type=jnp.float32)).astype(jnp.bfloat16)
    return after_attn + jnp.dot(hidden, w_down[level], preferred_element_type=jnp.float32)

def global_norm(rows, gain, bias):
    center = jnp.mean(rows)
    shifted = rows - center
    spread = jnp.mean(shifted * shifted)
    return gain * shifted * lax.rsqrt(spread + norm_eps) + bias

def reference(mixture, w_query, w_key, w_value, w_out, w_up, w_down, ln_gain, gln_gain, gln_bias):

    def intra_one(block_rows):
        return encoder_layer(block_rows, 0, w_query, w_key, w_value, w_out, w_up, w_down, ln_gain)

    def inter_one(sequence):
        return encoder_layer(sequence, 1, w_query, w_key, w_value, w_out, w_up, w_down, ln_gain)
    intra = lax.map(intra_one, mixture)
    intra_out = (global_norm(intra, gln_gain[0], gln_bias[0]) + mixture.astype(jnp.float32)).astype(jnp.bfloat16)
    across = jnp.transpose(intra_out, (1, 0, 2))
    inter = lax.map(inter_one, across)
    final = (global_norm(inter, gln_gain[1], gln_bias[1]) + across.astype(jnp.float32)).astype(jnp.bfloat16)
    return jnp.transpose(final, (1, 0, 2))
```

```python
import math

import jax
import jax.numpy as jnp
import numpy as np
from jax import lax
from jax.experimental import pallas as pl
from jax.experimental.pallas import tpu as pltpu
from jax.sharding import PartitionSpec as P

HEADS = 8
norm_eps = 1e-05
F32 = jnp.float32
BF16 = jnp.bfloat16


def pos_table(length, width):
    places = np.arange(length, dtype=np.float64)[:, None]
    column = np.arange(width)
    rates = np.exp(-(2 * (column // 2)) / width * math.log(10000.0))
    angles = places * rates[None, :]
    return np.where((column % 2 == 0)[None, :], np.sin(angles), np.cos(angles)).astype(np.float32)


def norm_rows(rows, gain):
    center = jnp.mean(rows, axis=-1, keepdims=True)
    shifted = rows - center
    spread = jnp.mean(shifted * shifted, axis=-1, keepdims=True)
    return shifted * lax.rsqrt(spread + norm_eps) * gain


def dot(a, b):
    return jnp.dot(a, b, preferred_element_type=F32)


def dot_nt(a, b):
    return lax.dot_general(a, b, (((1,), (1,)), ((), ())), preferred_element_type=F32)


def softmax_rows(scores, factor):
    top = jnp.max(scores, axis=-1, keepdims=True)
    powers = jnp.exp2((scores - top) * factor)
    return (powers * (1.0 / jnp.sum(powers, axis=-1, keepdims=True))).astype(BF16)


def attend(q, k, v):
    length, width = q.shape
    head_dim = width // HEADS
    factor = math.log2(math.e) / math.sqrt(head_dim)
    lane_head = lax.broadcasted_iota(jnp.int32, (1, width), 1) // head_dim

    def mask(test):
        return jnp.where(test, 1.0, 0.0).astype(BF16)

    total = None
    if length * 2 <= width and length % 128 == 0:
        half = HEADS // 2
        k_two = jnp.concatenate(
            [k * mask(lane_head < half), k * mask(lane_head >= half)], axis=0
        )
        for h in range(half):
            low, high = mask(lane_head == h), mask(lane_head == h + half)
            scores = dot_nt(q * (low + high), k_two)
            weights = jnp.concatenate(
                [softmax_rows(scores[:, :length], factor), softmax_rows(scores[:, length:], factor)],
                axis=1,
            )
            part = dot(weights, jnp.concatenate([v * low, v * high], axis=0))
            total = part if total is None else total + part
    else:
        for h in range(HEADS):
            own = mask(lane_head == h)
            weights = softmax_rows(dot_nt(q * own, k), factor)
            part = dot(weights, v * own)
            total = part if total is None else total + part
    return total.astype(BF16)


def layer_rows(x, count, level, refs):
    wq, wk, wv, wo, wu, wd, ln = refs
    length = x.shape[0] // count
    normed = norm_rows(x, ln[level, 0:1]).astype(BF16)
    q = dot(normed, wq[level]).astype(BF16)
    k = dot(normed, wk[level]).astype(BF16)
    v = dot(normed, wv[level]).astype(BF16)
    parts = []
    for g in range(count):
        rows = slice(g * length, (g + 1) * length)
        parts.append(attend(q[rows], k[rows], v[rows]))
    context = parts[0] if count == 1 else jnp.concatenate(parts, axis=0)
    after = x + dot(context, wo[level])
    normed = norm_rows(after, ln[level, 1:2]).astype(BF16)
    hidden = jnp.maximum(dot(normed, wu[level]), 0.0).astype(BF16)
    return after + dot(hidden, wd[level])


def fold(rows):
    return jnp.sum(rows.reshape(rows.shape[0] // 8, 8, rows.shape[1]), axis=0)


def layer_kernel(level, x_ref, pos_ref, *rest):
    refs, (out_ref, stat_ref) = rest[:7], rest[7:]
    count, length, width = x_ref.shape
    x = x_ref[...].astype(F32) + pos_ref[...][None]
    y = layer_rows(x.reshape(count * length, width), count, level, refs)
    out_ref[...] = y.astype(BF16).reshape(count, length, width)

    @pl.when(pl.program_id(0) == 0)
    def _():
        stat_ref[...] = jnp.zeros_like(stat_ref)

    stat_ref[0] += fold(y)
    stat_ref[1] += fold(y * y)


def run_layer(x, level, weights):
    total, length, width = x.shape
    count = max(1, min(total, 512 // length))
    pos = jnp.asarray(pos_table(length, width))
    whole = lambda a: pl.BlockSpec(a.shape, lambda i: (0,) * a.ndim)
    return pl.pallas_call(
        lambda *r: layer_kernel(level, *r),
        grid=(total // count,),
        out_shape=(
            jax.ShapeDtypeStruct(x.shape, BF16),
            jax.ShapeDtypeStruct((2, 8, width), F32),
        ),
        in_specs=[pl.BlockSpec((count, length, width), lambda i: (i, 0, 0)), whole(pos)]
        + [whole(w) for w in weights],
        out_specs=(
            pl.BlockSpec((count, length, width), lambda i: (i, 0, 0)),
            pl.BlockSpec((2, 8, width), lambda i: (0, 0, 0)),
        ),
        compiler_params=pltpu.CompilerParams(vmem_limit_bytes=60 * 2**20),
        name="layer%d" % level,
    )(x, pos, *weights)


def global_norm(rows, stats, gain, bias, shards):
    cells = float(rows.size * shards)
    sums = lax.psum(jnp.sum(stats, axis=(1, 2)), "span")
    center = sums[0] / cells
    spread = sums[1] / cells - center * center
    return gain * (rows.astype(F32) - center) * lax.rsqrt(spread + norm_eps) + bias


def body(mixture, wq, wk, wv, wo, wu, wd, ln, gln_gain, gln_bias):
    shards = lax.axis_size("span")
    weights = (wq, wk, wv, wo, wu, wd, ln)
    intra, stats = run_layer(mixture, 0, weights)
    intra_out = (
        global_norm(intra, stats, gln_gain[0], gln_bias[0], shards) + mixture.astype(F32)
    ).astype(BF16)
    moved = lax.all_to_all(intra_out, "span", split_axis=1, concat_axis=0, tiled=True)
    inter, stats = run_layer(jnp.swapaxes(moved, 0, 1), 1, weights)
    back = lax.all_to_all(inter, "span", split_axis=1, concat_axis=0, tiled=True)
    final = global_norm(back, stats, gln_gain[1], gln_bias[1], shards)
    return (jnp.swapaxes(final, 0, 1) + intra_out.astype(F32)).astype(BF16)


def solution(mesh):
    in_specs = (P(("mix", "span"), None, None), P(), P(), P(), P(), P(), P(), P(), P(), P())
    out_specs = P(("mix", "span"), None, None)
    return jax.shard_map(body, mesh=mesh, in_specs=in_specs, out_specs=out_specs, check_vma=False)
```

```python
import math

import jax
import jax.numpy as jnp
import numpy as np
from jax import lax
from jax.experimental import pallas as pl
from jax.experimental.pallas import tpu as pltpu
from jax.sharding import PartitionSpec as P

HEADS = 8
norm_eps = 1e-05
F32 = jnp.float32
BF16 = jnp.bfloat16


def pos_table(length, width):
    places = np.arange(length, dtype=np.float64)[:, None]
    column = np.arange(width)
    rates = np.exp(-(2 * (column // 2)) / width * math.log(10000.0))
    angles = places * rates[None, :]
    return np.where((column % 2 == 0)[None, :], np.sin(angles), np.cos(angles)).astype(np.float32)


def norm_rows(rows, gain):
    center = jnp.mean(rows, axis=-1, keepdims=True)
    shifted = rows - center
    spread = jnp.mean(shifted * shifted, axis=-1, keepdims=True)
    return shifted * lax.rsqrt(spread + norm_eps) * gain


def dot(a, b):
    return jnp.dot(a, b, preferred_element_type=F32)


def dot_nt(a, b):
    return lax.dot_general(a, b, (((1,), (1,)), ((), ())), preferred_element_type=F32)


def softmax_rows(scores, factor):
    top = jnp.max(scores, axis=-1, keepdims=True)
    powers = jnp.exp2((scores - top) * factor)
    return (powers * (1.0 / jnp.sum(powers, axis=-1, keepdims=True))).astype(BF16)


def attend(q, k, v):
    length, width = q.shape
    head_dim = width // HEADS
    factor = math.log2(math.e) / math.sqrt(head_dim)
    lane_head = lax.broadcasted_iota(jnp.int32, (1, width), 1) // head_dim

    def mask(test):
        return jnp.where(test, 1.0, 0.0).astype(BF16)

    total = None
    if length * 2 <= width and length % 128 == 0:
        half = HEADS // 2
        k_two = jnp.concatenate(
            [k * mask(lane_head < half), k * mask(lane_head >= half)], axis=0
        )
        for h in range(half):
            low, high = mask(lane_head == h), mask(lane_head == h + half)
            scores = dot_nt(q * (low + high), k_two)
            weights = jnp.concatenate(
                [softmax_rows(scores[:, :length], factor), softmax_rows(scores[:, length:], factor)],
                axis=1,
            )
            part = dot(weights, jnp.concatenate([v * low, v * high], axis=0))
            total = part if total is None else total + part
    else:
        for h in range(HEADS):
            own = mask(lane_head == h)
            weights = softmax_rows(dot_nt(q * own, k), factor)
            part = dot(weights, v * own)
            total = part if total is None else total + part
    return total.astype(BF16)


def layer_rows(x, count, level, refs):
    wq, wk, wv, wo, wu, wd, ln = refs
    length = x.shape[0] // count
    normed = norm_rows(x, ln[level, 0:1]).astype(BF16)
    q = dot(normed, wq[level]).astype(BF16)
    k = dot(normed, wk[level]).astype(BF16)
    v = dot(normed, wv[level]).astype(BF16)
    parts = []
    for g in range(count):
        rows = slice(g * length, (g + 1) * length)
        parts.append(attend(q[rows], k[rows], v[rows]))
    context = parts[0] if count == 1 else jnp.concatenate(parts, axis=0)
    after = x + dot(context, wo[level])
    normed = norm_rows(after, ln[level, 1:2]).astype(BF16)
    hidden = jnp.maximum(dot(normed, wu[level]), 0.0).astype(BF16)
    return after + dot(hidden, wd[level])


def fold(rows):
    return jnp.sum(rows.reshape(rows.shape[0] // 8, 8, rows.shape[1]), axis=0)


def peer_of(j, size):
    return lax.rem(lax.axis_index("span") + j, size)


def remote(src, dst, send_sem, recv_sem, peer):
    return pltpu.make_async_remote_copy(
        src_ref=src,
        dst_ref=dst,
        send_sem=send_sem,
        recv_sem=recv_sem,
        device_id={"span": peer},
        device_id_type=pl.DeviceIdType.MESH,
    )


def lanes_of(ref, rows):
    return jnp.concatenate([ref[c, rows, :] for c in range(ref.shape[0])], axis=1)


def block_kernel(
    n, halves, mix, wq_h, wk_h, wv_h, wo_h, wu_h, wd_h, ln, gain, bias, pos0, pos1, out,
    mix_v, mix_got, y_own, y_got, x_two, z_own, z_got, z_wide,
    wq, wk, wv, wo, wu, wd, stat, stat_own, stat_got,
    w_sem, mix_sem, keep_sem, mix_send, mix_recv, y_send, y_recv, z_send, z_recv,
    stat_send, stat_recv,
):
    me = lax.axis_index("span")
    segs, _, span_rows, width = mix.shape
    frames = n * halves * span_rows
    long = n * segs
    own_frames = halves * span_rows
    two = max(1, min(segs, 512 // frames))
    four = max(1, min(span_rows, 512 // long))
    cells = float(long * frames * width)

    loads = [
        [
            pltpu.make_async_copy(src.at[level], dst.at[level], w_sem.at[level, i])
            for i, (src, dst) in enumerate(
                ((wq_h, wq), (wk_h, wk), (wv_h, wv), (wo_h, wo), (wu_h, wu), (wd_h, wd))
            )
        ]
        for level in range(2)
    ]
    first = pltpu.make_async_copy(mix.at[:two], mix_v.at[:two], mix_sem.at[0])
    later = pltpu.make_async_copy(mix.at[two:], mix_v.at[two:], mix_sem.at[1])
    first.start()
    for load in loads[0]:
        load.start()
    later.start()

    barrier = pltpu.get_barrier_semaphore()
    for j in range(1, n):
        pl.semaphore_signal(
            barrier, inc=1, device_id={"span": peer_of(j, n)}, device_id_type=pl.DeviceIdType.MESH
        )
    pl.semaphore_wait(barrier, n - 1)

    def mix_copy(j, half):
        peer = peer_of(j, n)
        return remote(
            mix.at[:, peer * halves + half],
            mix_got.at[half, pl.ds(me * segs, segs)],
            mix_send.at[half, j],
            mix_recv.at[half, j],
            peer,
        )

    def keep_copy(half):
        return pltpu.make_async_copy(
            mix.at[:, me * halves + half],
            mix_got.at[half, pl.ds(me * segs, segs)],
            keep_sem.at[half],
        )

    for j in range(1, n):
        mix_copy(j, 0).start()
    for half in range(halves):
        keep_copy(half).start()
    for load in loads[1]:
        load.start()

    def y_copy(j, start, size):
        peer = peer_of(j, n)
        return remote(
            y_own.at[pl.ds(start, size), pl.ds(peer * halves, halves)],
            y_got.at[pl.ds(me * segs + start, size)],
            y_send.at[j],
            y_recv.at[j],
            peer,
        )

    def z_copy(j, start, size):
        peer = peer_of(j, n)
        return remote(
            z_own.at[pl.ds(start, size), peer],
            z_got.at[pl.ds(me * own_frames + start, size)],
            z_send.at[j],
            z_recv.at[j],
            peer,
        )

    def add_stats(rows):
        stat[0] += fold(rows)
        stat[1] += fold(rows * rows)

    def share_stats(which):
        total = jnp.sum(jnp.sum(stat[0], axis=0, keepdims=True), axis=1, keepdims=True)
        square = jnp.sum(jnp.sum(stat[1], axis=0, keepdims=True), axis=1, keepdims=True)
        row = lax.broadcasted_iota(jnp.int32, (8, 128), 0)
        tile = jnp.where(row == 0, total, square)
        stat_own[which] = tile
        stat_got[which, me] = tile
        stat[...] = jnp.zeros_like(stat)

    def stat_copy(which, j):
        return remote(
            stat_own.at[which],
            stat_got.at[which, me],
            stat_send.at[which, j],
            stat_recv.at[which, j],
            peer_of(j, n),
        )

    def read_stats(which):
        for j in range(1, n):
            stat_copy(which, j).wait()
        tile = jnp.sum(stat_got[which], axis=0)
        center = tile[0:1, 0:1] / cells
        spread = tile[1:2, 0:1] / cells - center * center
        return center, lax.rsqrt(spread + norm_eps)

    stat[...] = jnp.zeros_like(stat)
    first.wait()
    for load in loads[0]:
        load.wait()
    later.wait()
    refs = (wq, wk, wv, wo, wu, wd, ln)

    def intra_step(i, carry):
        @pl.when(i > 0)
        def _():
            for j in range(1, n):
                y_copy(j, (i - 1) * two, two).start()

        x = mix_v[pl.ds(i * two, two)].astype(F32).reshape(two, frames, width) + pos0[...][None]
        y = layer_rows(x.reshape(two * frames, width), two, 0, refs)
        y_own[pl.ds(i * two, two)] = y.astype(BF16).reshape(two, n * halves, span_rows, width)
        add_stats(y)
        return carry

    steps = segs // two
    lax.fori_loop(0, steps, intra_step, 0)
    share_stats(0)
    for j in range(1, n):
        stat_copy(0, j).start()
    for j in range(1, n):
        y_copy(j, (steps - 1) * two, two).start()
    for half in range(1, halves):
        for j in range(1, n):
            mix_copy(j, half).start()

    def keep_step(s, carry):
        y_got[me * segs + s] = y_own[s, pl.ds(me * halves, halves)]
        return carry

    lax.fori_loop(0, segs, keep_step, 0)
    for load in loads[1]:
        load.wait()
    center, scale = read_stats(0)

    def mid(rows, mixture):
        normed = gain[0:1] * (rows.astype(F32) - center) * scale + bias[0:1]
        return (normed + mixture.astype(F32)).astype(BF16).astype(F32)

    for j in range(1, n):
        y_copy(j, 0, segs).wait_recv()

    for half in range(halves):
        keep_copy(half).wait()
        for j in range(1, n):
            mix_copy(j, half).wait_recv()

        def turn_step(g, carry, half=half):
            for t in range(8):
                s = g * 8 + t
                rows = mid(y_got[s, half], mix_got[half, s])
                for c in range(width // 128):
                    x_two[c, pl.ds(s, span_rows, stride=long), :] = rows[:, c * 128 : c * 128 + 128]
            return carry

        lax.fori_loop(0, long // 8, turn_step, 0)

        def inter_step(i, carry, half=half):
            here = half * span_rows + i * four

            @pl.when(here > 0)
            def _():
                for j in range(1, n):
                    z_copy(j, here - four, four).start()

            x = lanes_of(x_two, pl.ds(i * four * long, four * long)).reshape(four, long, width)
            x = x + pos1[...][None]
            z = layer_rows(x.reshape(four * long, width), four, 1, refs)
            z_own[pl.ds(here, four)] = z.astype(BF16).reshape(four, n, segs, width)
            add_stats(z)
            return carry

        lax.fori_loop(0, span_rows // four, inter_step, 0)

    share_stats(1)
    for j in range(1, n):
        stat_copy(1, j).start()
    for j in range(1, n):
        z_copy(j, own_frames - four, four).start()

    def own_step(f, carry):
        z_got[me * own_frames + f] = z_own[f, me]
        return carry

    lax.fori_loop(0, own_frames, own_step, 0)
    center_two, scale_two = read_stats(1)
    for j in range(1, n):
        z_copy(j, 0, own_frames).wait_recv()

    def widen_step(f, carry):
        rows = z_got[pl.ds(f * 8, 8)].astype(F32).reshape(8 * segs, width)
        for c in range(width // 128):
            z_wide[c, pl.ds(f * 8 * segs, 8 * segs), :] = rows[:, c * 128 : c * 128 + 128]
        return carry

    lax.fori_loop(0, frames // 8, widen_step, 0)

    def final_step(s, carry):
        z = lanes_of(z_wide, pl.ds(s, frames, stride=segs))
        normed = gain[1:2] * (z - center_two) * scale_two + bias[1:2]
        shape = (frames, width)
        across = mid(y_own[s].reshape(shape), mix_v[s].reshape(shape))
        out[s] = (normed + across).astype(BF16).reshape(out.shape[1:])
        return carry

    lax.fori_loop(0, segs, final_step, 0)
    for j in range(1, n):
        for half in range(halves):
            mix_copy(j, half).wait_send()
        y_copy(j, 0, segs).wait_send()
        z_copy(j, 0, own_frames).wait_send()


def body(mixture, wq, wk, wv, wo, wu, wd, ln, gln_gain, gln_bias):
    n = lax.axis_size("span")
    segs, frames, width = mixture.shape
    own = frames // n
    halves = 2 if own % 32 == 0 else 1
    rows = own // halves
    long = n * segs
    mix = mixture.reshape(segs, n * halves, rows, width)
    pos0, pos1 = jnp.asarray(pos_table(frames, width)), jnp.asarray(pos_table(long, width))
    anywhere = pl.BlockSpec(memory_space=pl.ANY)
    vmem = pl.BlockSpec(memory_space=pltpu.VMEM)
    dma = pltpu.SemaphoreType.DMA
    weights = (wq, wk, wv, wo, wu, wd)
    result = pl.pallas_call(
        lambda *r: block_kernel(n, halves, *r),
        out_shape=jax.ShapeDtypeStruct(mix.shape, BF16),
        in_specs=[anywhere] * 7 + [vmem] * 5,
        out_specs=vmem,
        scratch_shapes=[
            pltpu.VMEM(mix.shape, BF16),
            pltpu.VMEM((halves, long, rows, width), BF16),
            pltpu.VMEM(mix.shape, BF16),
            pltpu.VMEM((long, halves, rows, width), BF16),
            pltpu.VMEM((width // 128, rows * long, 128), F32),
            pltpu.VMEM((own, n, segs, width), BF16),
            pltpu.VMEM((frames, segs, width), BF16),
            pltpu.VMEM((width // 128, frames * segs, 128), F32),
        ]
        + [pltpu.VMEM(w.shape, BF16) for w in weights]
        + [
            pltpu.VMEM((2, 8, width), F32),
            pltpu.VMEM((2, 8, 128), F32),
            pltpu.VMEM((2, n, 8, 128), F32),
            dma((2, 6)),
            dma((2,)),
            dma((halves,)),
            dma((halves, n)),
            dma((halves, n)),
            dma((n,)),
            dma((n,)),
            dma((n,)),
            dma((n,)),
            dma((2, n)),
            dma((2, n)),
        ],
        compiler_params=pltpu.CompilerParams(
            collective_id=0, has_side_effects=True, vmem_limit_bytes=62 * 2**20
        ),
        name="dual_path",
    )(mix, *weights, ln, gln_gain, gln_bias, pos0, pos1)
    return result.reshape(mixture.shape)


def solution(mesh):
    in_specs = (P(("mix", "span"), None, None), P(), P(), P(), P(), P(), P(), P(), P(), P())
    out_specs = P(("mix", "span"), None, None)
    return jax.shard_map(body, mesh=mesh, in_specs=in_specs, out_specs=out_specs, check_vma=False)
```

```python
import math

import jax
import jax.numpy as jnp
import numpy as np
from jax import lax
from jax.experimental import pallas as pl
from jax.experimental.pallas import tpu as pltpu
from jax.sharding import PartitionSpec as P

HEADS = 8
norm_eps = 1e-05
F32 = jnp.float32
BF16 = jnp.bfloat16


def pos_table(length, width):
    places = np.arange(length, dtype=np.float64)[:, None]
    column = np.arange(width)
    rates = np.exp(-(2 * (column // 2)) / width * math.log(10000.0))
    angles = places * rates[None, :]
    return np.where((column % 2 == 0)[None, :], np.sin(angles), np.cos(angles)).astype(np.float32)


def norm_rows(rows, gain):
    center = jnp.mean(rows, axis=-1, keepdims=True)
    shifted = rows - center
    spread = jnp.mean(shifted * shifted, axis=-1, keepdims=True)
    return shifted * lax.rsqrt(spread + norm_eps) * gain


def dot(a, b):
    return jnp.dot(a, b, preferred_element_type=F32)


def dot_nt(a, b):
    return lax.dot_general(a, b, (((1,), (1,)), ((), ())), preferred_element_type=F32)


def powers_of(scores, factor):
    top = jnp.max(scores, axis=-1, keepdims=True)
    return jnp.exp2((scores - top) * factor).astype(BF16)


def attend(q, k, v):
    length, width = q.shape
    head_dim = width // HEADS
    side = width // 2
    factor = math.log2(math.e) / math.sqrt(head_dim)
    lane_head = lax.broadcasted_iota(jnp.int32, (1, width), 1) // head_dim
    side_head = lax.broadcasted_iota(jnp.int32, (1, side), 1) // head_dim
    per_side = HEADS // 2

    def mask(test):
        return jnp.where(test, 1.0, 0.0).astype(BF16)

    def values_of(h):
        own = mask(side_head == h % per_side)
        start = (h // per_side) * side
        ones = jnp.broadcast_to(own, (length, side))
        return jnp.concatenate([v[:, start : start + side] * own, ones], axis=1)

    paired = length * 2 <= width and length % 128 == 0
    if paired:
        k_two = jnp.concatenate(
            [k * mask(lane_head % 2 == 0), k * mask(lane_head % 2 == 1)], axis=0
        )
    contexts = []
    for first in (0, per_side):
        total = None
        for h in range(first, first + per_side, 2 if paired else 1):
            if paired:
                scores = dot_nt(q * mask(lane_head // 2 == h // 2), k_two)
                weights = jnp.concatenate(
                    [powers_of(scores[:, :length], factor), powers_of(scores[:, length:], factor)],
                    axis=1,
                )
                part = dot(weights, jnp.concatenate([values_of(h), values_of(h + 1)], axis=0))
            else:
                weights = powers_of(dot_nt(q * mask(lane_head == h), k), factor)
                part = dot(weights, values_of(h))
            total = part if total is None else total + part
        contexts.append((total[:, :side] / total[:, side:]).astype(BF16))
    return jnp.concatenate(contexts, axis=1)


def layer_rows(x, count, level, refs):
    wq, wk, wv, wo, wu, wd, ln = refs
    length = x.shape[0] // count
    normed = norm_rows(x, ln[level, 0:1]).astype(BF16)
    q = dot(normed, wq[level]).astype(BF16)
    k = dot(normed, wk[level]).astype(BF16)
    v = dot(normed, wv[level]).astype(BF16)
    parts = []
    for g in range(count):
        rows = slice(g * length, (g + 1) * length)
        parts.append(attend(q[rows], k[rows], v[rows]))
    context = parts[0] if count == 1 else jnp.concatenate(parts, axis=0)
    after = x + dot(context, wo[level])
    normed = norm_rows(after, ln[level, 1:2]).astype(BF16)
    hidden = jnp.maximum(dot(normed, wu[level]), 0.0).astype(BF16)
    return after + dot(hidden, wd[level])


def fold(rows):
    return jnp.sum(rows.reshape(rows.shape[0] // 8, 8, rows.shape[1]), axis=0)


def peer_of(j, size):
    return lax.rem(lax.axis_index("span") + j, size)


def remote(src, dst, send_sem, recv_sem, peer):
    return pltpu.make_async_remote_copy(
        src_ref=src,
        dst_ref=dst,
        send_sem=send_sem,
        recv_sem=recv_sem,
        device_id={"span": peer},
        device_id_type=pl.DeviceIdType.MESH,
    )


def lanes_of(ref, rows):
    return jnp.concatenate([ref[c, rows, :] for c in range(ref.shape[0])], axis=1)


def block_kernel(
    n, halves, mix, wq_h, wk_h, wv_h, wo_h, wu_h, wd_h, ln, gain, bias, pos0, pos1, out,
    mix_v, mix_got, y_own, y_got, x_two, z_own, z_got, z_wide,
    wq, wk, wv, wo, wu, wd, stat, stat_own, stat_got,
    w_sem, mix_sem, keep_sem, mix_send, mix_recv, y_send, y_recv, z_send, z_recv,
    stat_send, stat_recv,
):
    me = lax.axis_index("span")
    segs, _, span_rows, width = mix.shape
    frames = n * halves * span_rows
    long = n * segs
    own_frames = halves * span_rows
    two = max(1, min(segs, 512 // frames))
    four = max(1, min(span_rows, 512 // long))
    cells = float(long * frames * width)

    loads = [
        [
            pltpu.make_async_copy(src.at[level], dst.at[level], w_sem.at[level, i])
            for i, (src, dst) in enumerate(
                ((wq_h, wq), (wk_h, wk), (wv_h, wv), (wo_h, wo), (wu_h, wu), (wd_h, wd))
            )
        ]
        for level in range(2)
    ]
    first = pltpu.make_async_copy(mix.at[:two], mix_v.at[:two], mix_sem.at[0])
    later = pltpu.make_async_copy(mix.at[two:], mix_v.at[two:], mix_sem.at[1])
    first.start()
    for load in loads[0]:
        load.start()
    later.start()

    barrier = pltpu.get_barrier_semaphore()
    for j in range(1, n):
        pl.semaphore_signal(
            barrier, inc=1, device_id={"span": peer_of(j, n)}, device_id_type=pl.DeviceIdType.MESH
        )
    pl.semaphore_wait(barrier, n - 1)

    def mix_copy(j, half):
        peer = peer_of(j, n)
        return remote(
            mix.at[:, peer * halves + half],
            mix_got.at[half, pl.ds(me * segs, segs)],
            mix_send.at[half, j],
            mix_recv.at[half, j],
            peer,
        )

    def keep_copy(half):
        return pltpu.make_async_copy(
            mix.at[:, me * halves + half],
            mix_got.at[half, pl.ds(me * segs, segs)],
            keep_sem.at[half],
        )

    for j in range(1, n):
        mix_copy(j, 0).start()
    for half in range(halves):
        keep_copy(half).start()
    for load in loads[1]:
        load.start()

    def y_copy(j, start, size):
        peer = peer_of(j, n)
        return remote(
            y_own.at[pl.ds(start, size), pl.ds(peer * halves, halves)],
            y_got.at[pl.ds(me * segs + start, size)],
            y_send.at[j],
            y_recv.at[j],
            peer,
        )

    def z_copy(j, start, size):
        peer = peer_of(j, n)
        return remote(
            z_own.at[pl.ds(start, size), peer],
            z_got.at[pl.ds(me * own_frames + start, size)],
            z_send.at[j],
            z_recv.at[j],
            peer,
        )

    def add_stats(rows):
        stat[0] += fold(rows)
        stat[1] += fold(rows * rows)

    def share_stats(which):
        total = jnp.sum(jnp.sum(stat[0], axis=0, keepdims=True), axis=1, keepdims=True)
        square = jnp.sum(jnp.sum(stat[1], axis=0, keepdims=True), axis=1, keepdims=True)
        row = lax.broadcasted_iota(jnp.int32, (8, 128), 0)
        tile = jnp.where(row == 0, total, square)
        stat_own[which] = tile
        stat_got[which, me] = tile
        stat[...] = jnp.zeros_like(stat)

    def stat_copy(which, j):
        return remote(
            stat_own.at[which],
            stat_got.at[which, me],
            stat_send.at[which, j],
            stat_recv.at[which, j],
            peer_of(j, n),
        )

    def read_stats(which):
        for j in range(1, n):
            stat_copy(which, j).wait()
        tile = jnp.sum(stat_got[which], axis=0)
        center = tile[0:1, 0:1] / cells
        spread = tile[1:2, 0:1] / cells - center * center
        return center, lax.rsqrt(spread + norm_eps)

    stat[...] = jnp.zeros_like(stat)
    first.wait()
    for load in loads[0]:
        load.wait()
    refs = (wq, wk, wv, wo, wu, wd, ln)

    def intra_step(i, carry):
        @pl.when(i == 1)
        def _():
            later.wait()

        @pl.when(i > 0)
        def _():
            for j in range(1, n):
                y_copy(j, (i - 1) * two, two).start()

        x = mix_v[pl.ds(i * two, two)].astype(F32).reshape(two, frames, width) + pos0[...][None]
        y = layer_rows(x.reshape(two * frames, width), two, 0, refs)
        y_own[pl.ds(i * two, two)] = y.astype(BF16).reshape(two, n * halves, span_rows, width)
        add_stats(y)
        return carry

    steps = segs // two
    lax.fori_loop(0, steps, intra_step, 0)
    share_stats(0)
    for j in range(1, n):
        stat_copy(0, j).start()
    for j in range(1, n):
        y_copy(j, (steps - 1) * two, two).start()
    for half in range(1, halves):
        for j in range(1, n):
            mix_copy(j, half).start()

    def keep_step(s, carry):
        y_got[me * segs + s] = y_own[s, pl.ds(me * halves, halves)]
        return carry

    lax.fori_loop(0, segs, keep_step, 0)
    for load in loads[1]:
        load.wait()
    center, scale = read_stats(0)

    def mid(rows, mixture):
        normed = gain[0:1] * (rows.astype(F32) - center) * scale + bias[0:1]
        return (normed + mixture.astype(F32)).astype(BF16).astype(F32)

    for j in range(1, n):
        y_copy(j, 0, segs).wait_recv()

    for half in range(halves):
        keep_copy(half).wait()
        for j in range(1, n):
            mix_copy(j, half).wait_recv()

        def turn_step(g, carry, half=half):
            for t in range(8):
                s = g * 8 + t
                rows = mid(y_got[s, half], mix_got[half, s])
                for c in range(width // 128):
                    x_two[c, pl.ds(s, span_rows, stride=long), :] = rows[:, c * 128 : c * 128 + 128]
            return carry

        lax.fori_loop(0, long // 8, turn_step, 0)

        def inter_step(i, carry, half=half):
            here = half * span_rows + i * four

            @pl.when(here > 0)
            def _():
                for j in range(1, n):
                    z_copy(j, here - four, four).start()

            x = lanes_of(x_two, pl.ds(i * four * long, four * long)).reshape(four, long, width)
            x = x + pos1[...][None]
            z = layer_rows(x.reshape(four * long, width), four, 1, refs)
            z_own[pl.ds(here, four)] = z.astype(BF16).reshape(four, n, segs, width)
            add_stats(z)
            return carry

        lax.fori_loop(0, span_rows // four, inter_step, 0)

    share_stats(1)
    for j in range(1, n):
        stat_copy(1, j).start()
    for j in range(1, n):
        z_copy(j, own_frames - four, four).start()

    def own_step(f, carry):
        z_got[me * own_frames + f] = z_own[f, me]
        return carry

    lax.fori_loop(0, own_frames, own_step, 0)
    center_two, scale_two = read_stats(1)
    for j in range(1, n):
        z_copy(j, 0, own_frames).wait_recv()

    def widen_step(f, carry):
        rows = z_got[pl.ds(f * 8, 8)].astype(F32).reshape(8 * segs, width)
        for c in range(width // 128):
            z_wide[c, pl.ds(f * 8 * segs, 8 * segs), :] = rows[:, c * 128 : c * 128 + 128]
        return carry

    lax.fori_loop(0, frames // 8, widen_step, 0)

    def final_step(s, carry):
        z = lanes_of(z_wide, pl.ds(s, frames, stride=segs))
        normed = gain[1:2] * (z - center_two) * scale_two + bias[1:2]
        shape = (frames, width)
        across = mid(y_own[s].reshape(shape), mix_v[s].reshape(shape))
        out[s] = (normed + across).astype(BF16).reshape(out.shape[1:])
        return carry

    lax.fori_loop(0, segs, final_step, 0)
    for j in range(1, n):
        for half in range(halves):
            mix_copy(j, half).wait_send()
        y_copy(j, 0, segs).wait_send()
        z_copy(j, 0, own_frames).wait_send()


def body(mixture, wq, wk, wv, wo, wu, wd, ln, gln_gain, gln_bias):
    n = lax.axis_size("span")
    segs, frames, width = mixture.shape
    own = frames // n
    halves = 2 if own % 32 == 0 else 1
    rows = own // halves
    long = n * segs
    mix = mixture.reshape(segs, n * halves, rows, width)
    pos0, pos1 = jnp.asarray(pos_table(frames, width)), jnp.asarray(pos_table(long, width))
    anywhere = pl.BlockSpec(memory_space=pl.ANY)
    vmem = pl.BlockSpec(memory_space=pltpu.VMEM)
    dma = pltpu.SemaphoreType.DMA
    weights = (wq, wk, wv, wo, wu, wd)
    result = pl.pallas_call(
        lambda *r: block_kernel(n, halves, *r),
        out_shape=jax.ShapeDtypeStruct(mix.shape, BF16),
        in_specs=[anywhere] * 7 + [vmem] * 5,
        out_specs=vmem,
        scratch_shapes=[
            pltpu.VMEM(mix.shape, BF16),
            pltpu.VMEM((halves, long, rows, width), BF16),
            pltpu.VMEM(mix.shape, BF16),
            pltpu.VMEM((long, halves, rows, width), BF16),
            pltpu.VMEM((width // 128, rows * long, 128), F32),
            pltpu.VMEM((own, n, segs, width), BF16),
            pltpu.VMEM((frames, segs, width), BF16),
            pltpu.VMEM((width // 128, frames * segs, 128), F32),
        ]
        + [pltpu.VMEM(w.shape, BF16) for w in weights]
        + [
            pltpu.VMEM((2, 8, width), F32),
            pltpu.VMEM((2, 8, 128), F32),
            pltpu.VMEM((2, n, 8, 128), F32),
            dma((2, 6)),
            dma((2,)),
            dma((halves,)),
            dma((halves, n)),
            dma((halves, n)),
            dma((n,)),
            dma((n,)),
            dma((n,)),
            dma((n,)),
            dma((2, n)),
            dma((2, n)),
        ],
        compiler_params=pltpu.CompilerParams(
            collective_id=0, has_side_effects=True, vmem_limit_bytes=62 * 2**20
        ),
        name="dual_path",
    )(mix, *weights, ln, gln_gain, gln_bias, pos0, pos1)
    return result.reshape(mixture.shape)


def solution(mesh):
    in_specs = (P(("mix", "span"), None, None), P(), P(), P(), P(), P(), P(), P(), P(), P())
    out_specs = P(("mix", "span"), None, None)
    return jax.shard_map(body, mesh=mesh, in_specs=in_specs, out_specs=out_specs, check_vma=False)
```
